32 devices in a mesh: group: 4 (over y, x), rank: 8 (over z, core).
Axes of the slice: x: 2, y: 2, z: 4, core: 2. Of those that a mesh axis runs over, the one named last changes fastest.
Arguments:
- queries: bfloat16 [8192, 2048], P(('group', 'rank')), may hold values from -32 to 32
- key_rows: bfloat16 [8192, 2048], P(('group', 'rank')), may hold values from -6 to 6
- value_rows: bfloat16 [8192, 2048], P(('group', 'rank')), may hold values from -6 to 6
- tile_links: int32 [64, 8], P(('group', 'rank')), may hold values from 0 to 15, as said below
- link_counts: int32 [64], P(('group', 'rank')), may hold values from 1 to 8, 256 in all
Outputs:
- attended: bfloat16 [8192, 2048], P(('group', 'rank'))
The draws below stay inside these ranges and needn't reach their ends.
Inputs may be any that keep to these rules, and one draw needn't show every extreme that they name: `tile_links`: each row names 8 different candidates.
All inputs are finite; a program needn't handle non-finite values. No bound on the sum of `link_counts` on one device may be relied on, other than what follows from the above.
Results may differ from the reference program's by a relative error of at most 0.0045.
Values may be sent and summed in bfloat16 or wider, within the bound.
A program may use at most 128 MiB of HBM per device.

```python
import math
import jax
import jax.numpy as jnp
import numpy as np
from jax import lax

H = 16
HD = 128
TILE = 128
TPD = 2
LMAX = 8
W = 2048
GROUPS = 4
RANKS = 8
NTILES = 64
NODES = 8192
CAND = 16


def shared_rows(key):
    base = jax.random.fold_in(key, 7)
    query_key, key_key = jax.random.split(base, 2)
    query_draw = jnp.clip(jax.random.normal(query_key, (NODES, W), jnp.float32), -6.0, 6.0)
    key_draw = jnp.clip(jax.random.normal(key_key, (NODES, W), jnp.float32), -6.0, 6.0)
    return (query_draw, key_draw)


def draw_queries(key, part):
    return shared_rows(key)[0].astype(jnp.bfloat16)


def draw_key_rows(key, part):
    return shared_rows(key)[1].astype(jnp.bfloat16)


def draw_tile_links(key, part):
    link_key = jax.random.fold_in(key, 11)
    scores = jax.random.randint(link_key, (NTILES, CAND), 0, 2 ** 20) * CAND + jnp.arange(CAND, dtype=jnp.int32)[None, :]
    order = jnp.argsort(scores, axis=1)
    return order[:, :LMAX].astype(jnp.int32)


def level_of(key, dims, cuts, smallest, high):
    factor_of, own = 1.0, jax.random.fold_in(key, 6)
    for dim, blocks in cuts:
        heights = jnp.exp(jax.random.uniform(jax.random.fold_in(own, dim), (blocks,), jnp.float32, smallest / len(cuts), high / len(cuts)))
        factor_of = factor_of * jnp.repeat(heights, dims[dim] // blocks).reshape([-1 if axis == dim else 1 for axis in range(len(dims))])
    return factor_of


def length_profile(amount, total, bound, lean):
    portions = [(1 << 20) // math.isqrt(standing ** lean) + 1 for standing in range(2, amount + 1)]
    spare, counts = total - bound - (amount - 1), [1] * (amount - 1)
    while spare > 0:
        candidates = [i for i in range(amount - 1) if counts[i] < bound]
        whole, left = sum([portions[i] for i in candidates]), spare
        for i in candidates:
            more = min(bound - counts[i], max(1, left * portions[i] // whole), spare)
            counts[i] = counts[i] + more
            spare = spare - more
    return np.array([bound] + counts)


def ragged(key, amount, total, limit, lean):
    if amount == 2:
        one = jax.random.randint(key, (), max(1, total - limit), min(limit, total - 1) + 1)
        return jnp.stack([one, total - one])
    lengths = jnp.asarray(length_profile(amount, total, limit, lean), jnp.int32)
    pairs = (amount - 1) // 2
    giver, sink = lengths[1:1 + 2 * pairs:2], lengths[2:2 + 2 * pairs:2]
    room = jnp.minimum(giver - 1, limit - sink)
    passed = jax.random.randint(jax.random.fold_in(key, 1), (pairs,), 0, 1 << 20) % (room + 1)
    lengths = lengths.at[1:1 + 2 * pairs:2].set(giver - passed).at[2:2 + 2 * pairs:2].set(sink + passed)
    return lengths[jax.random.permutation(jax.random.fold_in(key, 2), amount)]


def centred(key, dims, scale, limit, cuts=(), kind=jnp.bfloat16):
    values = jax.random.normal(key, dims, jnp.float32) * scale
    if len(cuts) > 0:
        values = level_of(key, dims, cuts, -0.22, 0.18) * values
    return jnp.clip(values, min=-limit, max=limit).astype(kind)


def setup_inputs(seed: int = 0) -> dict:
    splits = jax.random.split(jax.random.key(seed), 6)
    queries = draw_queries(jax.random.fold_in(splits[5], 71), 0)
    key_rows = draw_key_rows(jax.random.fold_in(splits[5], 71), 0)
    value_rows = centred(splits[2], (NODES, W), 1.0, 6.0, ((0, 32),))
    tile_links = draw_tile_links(jax.random.fold_in(splits[5], 71), 0)
    link_counts = ragged(splits[4], NTILES, NTILES * LMAX // 2, LMAX, 2).astype(jnp.int32)
    return dict(queries=queries, key_rows=key_rows, value_rows=value_rows, tile_links=tile_links, link_counts=link_counts)


def candidate_tiles(tile_id, slot_ids):
    device = tile_id // TPD
    group_id = device // RANKS
    range_id = device % RANKS
    within = slot_ids % TPD
    block_id = slot_ids // TPD
    offsets = jnp.array([-2, -1, 1, 2], jnp.int32)
    beside = offsets[jnp.clip(block_id - 1, 0, 3)]
    beside_range = (range_id + beside) % RANKS
    peer_group = (group_id + block_id - 4) % GROUPS
    local_tile = device * TPD + within
    beside_tile = (group_id * RANKS + beside_range) * TPD + within
    peer_tile = (peer_group * RANKS + range_id) * TPD + within
    chosen = jnp.where(block_id == 0, local_tile, jnp.where(block_id <= 4, beside_tile, peer_tile))
    return chosen.astype(jnp.int32)


def softmax_mix(query_tile, chosen_keys, chosen_values, usable):
    scores = jnp.einsum("qhd,khd->hqk", query_tile, chosen_keys) * (HD ** -0.5)
    key_mask = jnp.repeat(usable, TILE)
    scores = jnp.where(key_mask[None, None, :], scores, -jnp.inf)
    row_max = jnp.max(scores, axis=-1, keepdims=True)
    weights = jnp.exp(scores - row_max)
    row_total = jnp.sum(weights, axis=-1)
    rounded = weights.astype(jnp.bfloat16)
    mixed_rows = jnp.einsum("hqk,khd->qhd", rounded.astype(jnp.float32), chosen_values)
    return (mixed_rows / jnp.transpose(row_total)[:, :, None]).reshape(TILE, W).astype(jnp.bfloat16)


def reference(queries, key_rows, value_rows, tile_links, link_counts):
    key_tiles = key_rows.reshape(NTILES, TILE, W)
    value_tiles = value_rows.reshape(NTILES, TILE, W)

    def one_tile(tile_id):
        first = jnp.reshape(tile_id % TPD, (1,)).astype(jnp.int32)
        slot_ids = jnp.concatenate([first, tile_links[tile_id].astype(jnp.int32)])
        global_ids = candidate_tiles(tile_id, slot_ids)
        chosen_keys = key_tiles[global_ids].reshape((LMAX + 1) * TILE, H, HD).astype(jnp.float32)
        chosen_values = value_tiles[global_ids].reshape((LMAX + 1) * TILE, H, HD).astype(jnp.float32)
        query_tile = lax.dynamic_slice_in_dim(queries, (tile_id * TILE).astype(jnp.int32), TILE, 0)
        query_tile = query_tile.reshape(TILE, H, HD).astype(jnp.float32)
        usable = jnp.concatenate([jnp.ones((1,), bool), jnp.arange(LMAX, dtype=jnp.int32) < link_counts[tile_id]])
        return softmax_mix(query_tile, chosen_keys, chosen_values, usable)

    result = lax.map(one_tile, jnp.arange(NTILES, dtype=jnp.int32))
    return result.reshape(NODES, W)
```

```python
import functools
import math

import jax
import jax.numpy as jnp
from jax import lax
from jax.experimental import pallas as pl
from jax.experimental.pallas import tpu as pltpu
from jax.sharding import PartitionSpec as P

HD = 128
HEADS_PER_CHUNK = 2
WINDOW = 3
MESH = pl.DeviceIdType.MESH


def kernel(
    groups,
    ranks,
    q_hbm,
    k_hbm,
    v_hbm,
    links,
    counts,
    o_ref,
    land,
    q_v,
    bias,
    send_sems,
    recv_sems,
    q_sem,
):
    chunks, _, slots, rows, width = land.shape
    tiles, lmax = links.shape
    tile_rows = rows // tiles
    g = lax.axis_index("group")
    r = lax.axis_index("rank")
    core = lax.rem(r, 2)
    partner = (g, r + 1 - 2 * core)
    ahead = (g, lax.rem(r + 2, ranks))
    behind = (g, lax.rem(r + ranks - 2, ranks))
    flows = [(ahead, 1), (behind, 4)]
    for step in range(1, groups):
        flows.append(((lax.rem(g + groups - step, groups), r), 4 + step))
    flows.append((partner, 2 + core))
    relay = len(flows)

    barrier = pltpu.get_barrier_semaphore()
    for device, _ in flows:
        pl.semaphore_signal(barrier, inc=1, device_id=device, device_id_type=MESH)

    def columns(c):
        return pl.ds(pl.multiple_of(c * width, width), width)

    def own_copy(c, kv):
        src = (k_hbm, v_hbm)[kv]
        return pltpu.make_async_copy(
            src.at[:, columns(c)], land.at[c, kv, 0], recv_sems.at[c, kv, 0]
        )

    def flow_copy(c, kv, f):
        device, slot = flows[f]
        src = (k_hbm, v_hbm)[kv]
        return pltpu.make_async_remote_copy(
            src_ref=src.at[:, columns(c)],
            dst_ref=land.at[c, kv, slot],
            send_sem=send_sems.at[c, kv, f],
            recv_sem=recv_sems.at[c, kv, slot],
            device_id=device,
            device_id_type=MESH,
        )

    def relay_copy(c, kv):
        return pltpu.make_async_remote_copy(
            src_ref=land.at[c, kv, 4 - 3 * core],
            dst_ref=land.at[c, kv, 3 - core],
            send_sem=send_sems.at[c, kv, relay],
            recv_sem=recv_sems.at[c, kv, 3 - core],
            device_id=partner,
            device_id_type=MESH,
        )

    def arrived(c, kv, slot):
        pltpu.make_async_remote_copy(
            src_ref=land.at[c, kv, slot],
            dst_ref=land.at[c, kv, slot],
            send_sem=send_sems.at[c, kv, 0],
            recv_sem=recv_sems.at[c, kv, slot],
            device_id=partner,
            device_id_type=MESH,
        ).wait_recv()

    def issue(c):
        for kv in range(2):
            for f in range(len(flows)):
                flow_copy(c, kv, f).start()

    q_copy = pltpu.make_async_copy(q_hbm, q_v, q_sem)
    q_copy.start()
    pl.semaphore_wait(barrier, len(flows))

    @pl.loop(0, min(WINDOW, chunks))
    def _(c):
        issue(c)

    @pl.loop(0, chunks)
    def _(c):
        for kv in range(2):
            own_copy(c, kv).start()

    cand = lax.broadcasted_iota(jnp.int32, (1, slots * rows), 1) // tile_rows
    for i in range(tiles):
        used = jnp.where(cand == i, 1, 0)
        for j in range(lmax):
            hit = jnp.where(j < counts[i], links[i, j], -1)
            used = used + jnp.where(cand == hit, 1, 0)
        bias[i, :, :] = jnp.where(used == 0, -jnp.inf, jnp.where(used == 2, 1.0, 0.0))
    q_copy.wait()

    scale = HD ** (-0.5) * math.log2(math.e)

    def attend(c):
        for h in range(width // HD):
            cols = slice(h * HD, (h + 1) * HD)
            keys = land[c, 0, :, :, cols].reshape(slots * rows, HD)
            values = land[c, 1, :, :, cols].reshape(slots * rows, HD)
            head = pl.ds(pl.multiple_of(c * width + h * HD, HD), HD)
            scores = lax.dot_general(
                q_v[:, head], keys, (((1,), (1,)), ((), ())), preferred_element_type=jnp.float32
            )
            scores = scores.reshape(tiles, tile_rows, slots * rows) * scale + bias[...]
            scores = scores.reshape(rows, slots * rows)
            weights = jnp.exp2(scores - jnp.max(scores, axis=1, keepdims=True))
            total = jnp.sum(weights, axis=1, keepdims=True)
            mixed = jnp.dot(
                weights.astype(jnp.bfloat16), values, preferred_element_type=jnp.float32
            )
            o_ref[:, head] = (mixed / total).astype(jnp.bfloat16)

    @pl.loop(0, chunks + 1)
    def _(c):
        @pl.when(c < chunks)
        def _():
            for kv in range(2):
                arrived(c, kv, 4 - 3 * core)
                relay_copy(c, kv).start()

        @pl.when(c + WINDOW < chunks)
        def _():
            issue(c + WINDOW)

        @pl.when(c >= 1)
        def _():
            b = c - 1
            for kv in range(2):
                own_copy(b, kv).wait()
                arrived(b, kv, 1 + 3 * core)
                for slot in (2, 3) + tuple(range(5, slots)):
                    arrived(b, kv, slot)
            attend(b)

    @pl.loop(0, chunks)
    def _(c):
        for kv in range(2):
            for f in range(len(flows)):
                flow_copy(c, kv, f).wait_send()
            relay_copy(c, kv).wait_send()


def shards(groups, ranks, queries, key_rows, value_rows, tile_links, link_counts):
    rows, features = queries.shape
    tiles = tile_links.shape[0]
    slots = 4 + groups
    width = HEADS_PER_CHUNK * HD
    chunks = features // width
    hbm = pl.BlockSpec(memory_space=pl.ANY)
    smem = pl.BlockSpec(memory_space=pltpu.SMEM)
    return pl.pallas_call(
        functools.partial(kernel, groups, ranks),
        out_shape=jax.ShapeDtypeStruct((rows, features), jnp.bfloat16),
        in_specs=[hbm, hbm, hbm, smem, smem],
        out_specs=pl.BlockSpec(memory_space=pltpu.VMEM),
        scratch_shapes=[
            pltpu.VMEM((chunks, 2, slots, rows, width), jnp.bfloat16),
            pltpu.VMEM((rows, features), jnp.bfloat16),
            pltpu.VMEM((tiles, 1, slots * rows), jnp.float32),
            pltpu.SemaphoreType.DMA((chunks, 2, groups + 3)),
            pltpu.SemaphoreType.DMA((chunks, 2, slots + 1)),
            pltpu.SemaphoreType.DMA,
        ],
        compiler_params=pltpu.CompilerParams(
            collective_id=0, has_side_effects=True, vmem_limit_bytes=48 * 2**20
        ),
    )(queries, key_rows, value_rows, tile_links, link_counts)


def solution(mesh):
    nodes = P(("group", "rank"), None)
    return jax.shard_map(
        functools.partial(shards, mesh.shape["group"], mesh.shape["rank"]),
        mesh=mesh,
        in_specs=(nodes, nodes, nodes, nodes, P(("group", "rank"))),
        out_specs=nodes,
        check_vma=False,
    )
```

```python
import functools
import math

import jax
import jax.numpy as jnp
from jax import lax
from jax.experimental import pallas as pl
from jax.experimental.pallas import tpu as pltpu
from jax.sharding import PartitionSpec as P

HD = 128
CHUNK_SIXTEENTHS = (4, 4, 4, 2, 1, 1)
MESH = pl.DeviceIdType.MESH


def kernel(
    groups,
    ranks,
    bounds,
    q_hbm,
    k_hbm,
    v_hbm,
    links_hbm,
    counts_hbm,
    o_ref,
    land,
    q_v,
    bias,
    send_sems,
    recv_sems,
    q_sem,
    links,
    counts,
    list_sems,
):
    _, slots, rows, _ = land.shape
    chunks = len(bounds) - 1
    tiles, lmax = links.shape
    tile_rows = rows // tiles
    g = lax.axis_index("group")
    r = lax.axis_index("rank")
    core = lax.rem(r, 2)
    partner = (g, r + 1 - 2 * core)
    upper = (2 * r) // ranks
    first = (g, lax.rem(r + ranks - 2 + 4 * upper, ranks))
    second = (g, lax.rem(r + ranks + 2 - 4 * upper, ranks))
    flows = [(first, 4 - 3 * upper), (second, 1 + 3 * upper)]
    crossed = groups == 4
    across = (g + 1 - 2 * lax.rem(g, 2), lax.rem(g + 2, 4))

    def peer_slot(source, at):
        return 4 + lax.rem(source - at + groups, groups)

    if crossed:
        for near in across:
            flows.append(((near, r), peer_slot(g, near)))
    else:
        for step in range(1, groups):
            flows.append(((lax.rem(g + groups - step, groups), r), 4 + step))
    flows.append((partner, 2 + core))
    relay = len(flows)
    hops = (across, across[::-1])

    barrier = pltpu.get_barrier_semaphore()
    for device, _ in flows:
        pl.semaphore_signal(barrier, inc=1, device_id=device, device_id_type=MESH)

    def columns(c):
        return pl.ds(bounds[c] * HD, (bounds[c + 1] - bounds[c]) * HD)

    def own_copy(c, kv):
        src = (k_hbm, v_hbm)[kv]
        return pltpu.make_async_copy(
            src.at[:, columns(c)], land.at[kv, 0, :, columns(c)], recv_sems.at[c, kv, 0]
        )

    def flow_copy(c, kv, f):
        device, slot = flows[f]
        src = (k_hbm, v_hbm)[kv]
        return pltpu.make_async_remote_copy(
            src_ref=src.at[:, columns(c)],
            dst_ref=land.at[kv, slot, :, columns(c)],
            send_sem=send_sems.at[c, kv, f],
            recv_sem=recv_sems.at[c, kv, slot],
            device_id=device,
            device_id_type=MESH,
        )

    def relay_copy(c, kv):
        return pltpu.make_async_remote_copy(
            src_ref=land.at[kv, 4 - 3 * core, :, columns(c)],
            dst_ref=land.at[kv, 3 - core, :, columns(c)],
            send_sem=send_sems.at[c, kv, relay],
            recv_sem=recv_sems.at[c, kv, 3 - core],
            device_id=partner,
            device_id_type=MESH,
        )

    def cross_copy(c, kv):
        source, target = hops[kv]
        slot = peer_slot(source, target)
        return pltpu.make_async_remote_copy(
            src_ref=land.at[kv, peer_slot(source, g), :, columns(c)],
            dst_ref=land.at[kv, slot, :, columns(c)],
            send_sem=send_sems.at[c, kv, relay + 1],
            recv_sem=recv_sems.at[c, kv, slot],
            device_id=(target, r),
            device_id_type=MESH,
        )

    def arrived(c, kv, slot):
        pltpu.make_async_remote_copy(
            src_ref=land.at[kv, slot, :, columns(c)],
            dst_ref=land.at[kv, slot, :, columns(c)],
            send_sem=send_sems.at[c, kv, 0],
            recv_sem=recv_sems.at[c, kv, slot],
            device_id=partner,
            device_id_type=MESH,
        ).wait_recv()

    def issue(c):
        for kv in range(2):
            for f in range(len(flows)):
                flow_copy(c, kv, f).start()

    local = [
        pltpu.make_async_copy(q_hbm, q_v, q_sem),
        pltpu.make_async_copy(links_hbm, links, list_sems.at[0]),
        pltpu.make_async_copy(counts_hbm, counts, list_sems.at[1]),
    ]
    for copy in local:
        copy.start()
    pl.semaphore_wait(barrier, len(flows))

    for c in range(chunks):
        issue(c)
    for c in range(chunks):
        for kv in range(2):
            own_copy(c, kv).start()

    for copy in local:
        copy.wait()
    cand = lax.broadcasted_iota(jnp.int32, (1, slots * rows), 1) // tile_rows
    for i in range(tiles):
        used = jnp.where(cand == i, 1, 0)
        for j in range(lmax):
            hit = jnp.where(j < counts[i], links[i, j], -1)
            used = used + jnp.where(cand == hit, 1, 0)
        bias[i, :, :] = jnp.where(used == 0, -jnp.inf, jnp.where(used == 2, 1.0, 0.0))

    scale = HD ** (-0.5) * math.log2(math.e)

    def attend(c):
        @pl.loop(bounds[c], bounds[c + 1])
        def _(h):
            head = pl.ds(pl.multiple_of(h * HD, HD), HD)
            keys = land[0, :, :, head].reshape(slots * rows, HD)
            values = land[1, :, :, head].reshape(slots * rows, HD)
            scores = lax.dot_general(
                q_v[:, head], keys, (((1,), (1,)), ((), ())), preferred_element_type=jnp.float32
            )
            scores = scores.reshape(tiles, tile_rows, slots * rows) * scale + bias[...]
            scores = scores.reshape(rows, slots * rows)
            weights = jnp.exp2(scores - jnp.max(scores, axis=1, keepdims=True))
            total = jnp.sum(weights, axis=1, keepdims=True)
            mixed = jnp.dot(
                weights.astype(jnp.bfloat16), values, preferred_element_type=jnp.float32
            )
            o_ref[:, head] = (mixed / total).astype(jnp.bfloat16)

    for c in range(chunks + 1):
        if c < chunks:
            for kv in range(2):
                arrived(c, kv, 4 - 3 * core)
                relay_copy(c, kv).start()
                if crossed:
                    arrived(c, kv, peer_slot(hops[kv][0], g))
                    cross_copy(c, kv).start()
        if c >= 1:
            b = c - 1
            for kv in range(2):
                own_copy(b, kv).wait()
                arrived(b, kv, 1 + 3 * core)
                for slot in (2, 3):
                    arrived(b, kv, slot)
                if crossed:
                    arrived(b, kv, peer_slot(hops[kv][1], g))
                    arrived(b, kv, peer_slot(3 - g, g))
                else:
                    for slot in range(5, slots):
                        arrived(b, kv, slot)
            attend(b)

    for c in range(chunks):
        for kv in range(2):
            for f in range(len(flows)):
                flow_copy(c, kv, f).wait_send()
            relay_copy(c, kv).wait_send()
            if crossed:
                cross_copy(c, kv).wait_send()


def shards(groups, ranks, queries, key_rows, value_rows, tile_links, link_counts):
    rows, features = queries.shape
    tiles = tile_links.shape[0]
    slots = 4 + groups
    heads = features // HD
    bounds = [0]
    for part in CHUNK_SIXTEENTHS:
        bounds.append(bounds[-1] + part * heads // 16)
    chunks = len(bounds) - 1
    hbm = pl.BlockSpec(memory_space=pl.ANY)
    return pl.pallas_call(
        functools.partial(kernel, groups, ranks, tuple(bounds)),
        out_shape=jax.ShapeDtypeStruct((rows, features), jnp.bfloat16),
        in_specs=[hbm] * 5,
        out_specs=pl.BlockSpec(memory_space=pltpu.VMEM),
        scratch_shapes=[
            pltpu.VMEM((2, slots, rows, features), jnp.bfloat16),
            pltpu.VMEM((rows, features), jnp.bfloat16),
            pltpu.VMEM((tiles, 1, slots * rows), jnp.float32),
            pltpu.SemaphoreType.DMA((chunks, 2, groups + 4)),
            pltpu.SemaphoreType.DMA((chunks, 2, slots + 1)),
            pltpu.SemaphoreType.DMA,
            pltpu.SMEM(tile_links.shape, jnp.int32),
            pltpu.SMEM(link_counts.shape, jnp.int32),
            pltpu.SemaphoreType.DMA((2,)),
        ],
        compiler_params=pltpu.CompilerParams(
            collective_id=0, has_side_effects=True, vmem_limit_bytes=62 * 2**20
        ),
    )(queries, key_rows, value_rows, tile_links, link_counts)


def solution(mesh):
    nodes = P(("group", "rank"), None)
    return jax.shard_map(
        functools.partial(shards, mesh.shape["group"], mesh.shape["rank"]),
        mesh=mesh,
        in_specs=(nodes, nodes, nodes, nodes, P(("group", "rank"))),
        out_specs=nodes,
        check_vma=False,
    )
```
